32 devices in a mesh: outer: 4 (over y, core), inner: 8 (over z, x).
Axes of the slice: x: 2, y: 2, z: 4, core: 2. Of those that a mesh axis runs over, the one named last changes fastest.
Arguments:
- query_rows: bfloat16 [8192, 1024], P(('outer', 'inner')), may hold values from -6 to 6
- key_rows: bfloat16 [8192, 1024], P(('outer', 'inner')), may hold values from -6 to 6
- value_rows: bfloat16 [8192, 1024], P(('outer', 'inner')), may hold values from -6 to 6
- log_decay: float32 [8, 8192], P(None, ('outer', 'inner')), may hold values from -0.8 to 0, as said below
- grad_out: bfloat16 [8192, 1024], P(('outer', 'inner')), may hold values from -6 to 6
Outputs:
- attended: bfloat16 [8192, 1024], P(('outer', 'inner'))
- grad_queries: bfloat16 [8192, 1024], P(('outer', 'inner'))
- grad_keys: bfloat16 [8192, 1024], P(('outer', 'inner'))
- grad_values: bfloat16 [8192, 1024], P(('outer', 'inner'))
The draws below stay inside these ranges and needn't reach their ends.
Inputs may be any that keep to these rules, and one draw needn't show every extreme that they name: `log_decay`: every entry is negative.
All inputs are finite; a program needn't handle non-finite values.
Results may differ from the reference program's by a relative error of at most 0.0063.
Values sent between devices are 32-bit elements; how exact they have to be, the bound alone decides.
A program may use at most 320 MiB of HBM per device.

```python
import math
import jax
import jax.numpy as jnp
from jax import lax

HALF_HEADS = 8
E = 128
TOK_DEV = 256
SEQUENCE_TOKENS = 8192


def draw_log_decay(key, part):
    random_subkeys = jax.random.split(jax.random.fold_in(key, 17), 7)
    ranking = jax.random.permutation(random_subkeys[0], HALF_HEADS)
    fast_count = HALF_HEADS // 2
    fast_head_flags = ranking < fast_count
    fast_rate = jnp.exp(jax.random.uniform(random_subkeys[1], (HALF_HEADS,), jnp.float32, jnp.log(5.0), jnp.log(50.0))) / SEQUENCE_TOKENS
    slow_rate = jnp.exp(jax.random.uniform(random_subkeys[2], (HALF_HEADS,), jnp.float32, jnp.log(0.05), jnp.log(0.25))) / SEQUENCE_TOKENS
    base_rate = jnp.where(fast_head_flags, fast_rate, slow_rate)
    blocks = SEQUENCE_TOKENS // TOK_DEV
    block_factor = jax.random.uniform(random_subkeys[3], (HALF_HEADS, blocks), jnp.float32, 0.5, 2.0)
    block_factor = jnp.repeat(block_factor, TOK_DEV, axis=1)
    token_factor = jax.random.uniform(random_subkeys[4], (HALF_HEADS, SEQUENCE_TOKENS), jnp.float32, 0.5, 1.5)
    decay_rates = base_rate[:, None] * block_factor * token_factor
    spike_position = jax.random.randint(random_subkeys[5], (HALF_HEADS, 2), 0, SEQUENCE_TOKENS)
    spike_length = jax.random.uniform(random_subkeys[6], (HALF_HEADS, 2), jnp.float32, jnp.log(0.5), jnp.log(0.8))
    token_positions = jnp.arange(SEQUENCE_TOKENS, dtype=jnp.int32)
    spike_flags = token_positions[None, None, :] == spike_position[:, :, None]
    decay_spikes = jnp.sum(jnp.where(spike_flags, spike_length[:, :, None], 0.0), axis=1)
    decay_spikes = jnp.where(fast_head_flags[:, None], 0.0, decay_spikes)
    return (decay_spikes - decay_rates).astype(jnp.float32)


def steps_of(stream_key, shape, cuts, least, largest):
    def one(axis_at, parts):
        draws = jax.random.uniform(jax.random.fold_in(jax.random.fold_in(stream_key, 6), axis_at), (parts,), jnp.float32, least / len(cuts), largest / len(cuts))
        return jnp.repeat(jnp.exp(draws), shape[axis_at] // parts).reshape((-1,) + (1,) * (len(shape) - axis_at - 1))

    factor_of = one(*cuts[0])
    for cut in cuts[1:]:
        factor_of = factor_of * one(*cut)
    return factor_of


def scatter_about(rng, shape, deviation, limit, shards=(), kind=jnp.bfloat16):
    drawn = deviation * jax.random.normal(rng, shape, jnp.float32)
    if shards:
        drawn = drawn * steps_of(rng, shape, shards, -0.22, 0.18)
    return jnp.clip(drawn, -limit, limit).astype(kind)


def setup_inputs(seed: int = 0) -> dict:
    streams_of = jax.random.split(jax.random.key(seed), 6)
    query_rows = scatter_about(streams_of[0], (SEQUENCE_TOKENS, HALF_HEADS * E), 1.0, 6.0, ((0, 32),))
    key_rows = scatter_about(streams_of[1], (SEQUENCE_TOKENS, HALF_HEADS * E), 1.0, 6.0, ((0, 32),))
    value_rows = scatter_about(streams_of[2], (SEQUENCE_TOKENS, HALF_HEADS * E), 1.0, 6.0, ((0, 32),))
    log_decay = draw_log_decay(jax.random.fold_in(streams_of[5], 71), 0)
    grad_out = scatter_about(streams_of[4], (SEQUENCE_TOKENS, HALF_HEADS * E), 1.0, 6.0, ((0, 32),))
    return dict(query_rows=query_rows, key_rows=key_rows, value_rows=value_rows, log_decay=log_decay, grad_out=grad_out)


EPSILON = 1e-06

def causal_decay(running):
    length_rows = running.shape[1]
    row_index = lax.broadcasted_iota(jnp.int32, (length_rows, length_rows), 0)
    col_index = lax.broadcasted_iota(jnp.int32, (length_rows, length_rows), 1)
    causal = (col_index <= row_index)[None]
    gaps = running[:, :, None] - running[:, None, :]
    return jnp.where(causal, jnp.exp(jnp.where(causal, gaps, 0.0)), 0.0)

def block_terms(query_block, key_block, decays, scaling):
    running = jnp.cumsum(decays, axis=1)
    totals = running[:, -1]
    growth = jnp.exp(running).T[:, :, None]
    shrink = jnp.exp(totals[:, None] - running).T[:, :, None]
    query_dec = (query_block.astype(jnp.float32) * growth).astype(jnp.bfloat16)
    key_dec = (key_block.astype(jnp.float32) * shrink).astype(jnp.bfloat16)
    decay_mat = causal_decay(running)
    scores = jnp.einsum('the,she->hts', query_block.astype(jnp.float32), key_block.astype(jnp.float32))
    weights = (scores * scaling * decay_mat).astype(jnp.bfloat16)
    return (totals, growth, shrink, query_dec, key_dec, decay_mat, weights)

def reference(query_rows, key_rows, value_rows, log_decay, grad_out):
    blocks = SEQUENCE_TOKENS // TOK_DEV
    scaling = 1.0 / math.sqrt(E)
    block_shape = (blocks, TOK_DEV, HALF_HEADS, E)
    query_all = query_rows.reshape(block_shape)
    key_all = key_rows.reshape(block_shape)
    value_all = value_rows.reshape(block_shape)
    grad_all = grad_out.reshape(block_shape)
    decay_all = log_decay.reshape(HALF_HEADS, blocks, TOK_DEV).transpose(1, 0, 2)

    def forward_step(carry_state, inputs):
        query_block, key_block, value_block, decays = inputs
        totals, growth, shrink, query_dec, key_dec, decay_mat, weights = block_terms(query_block, key_block, decays, scaling)
        local_state = jnp.einsum('the,thf->hef', key_dec.astype(jnp.float32), value_block.astype(jnp.float32))
        new_state = jnp.exp(totals)[:, None, None] * carry_state + local_state
        return (new_state, carry_state.astype(jnp.bfloat16))
    start_state = jnp.zeros((HALF_HEADS, E, E), jnp.float32)
    _, entering = lax.scan(forward_step, start_state, (query_all, key_all, value_all, decay_all))

    def backward_step(later_state, inputs):
        query_block, key_block, value_block, decays, entering_half, grad_block = inputs
        totals, growth, shrink, query_dec, key_dec, decay_mat, weights = block_terms(query_block, key_block, decays, scaling)
        value_float = value_block.astype(jnp.float32)
        entering_float = entering_half.astype(jnp.float32)
        mixed = jnp.einsum('hts,shf->thf', weights.astype(jnp.float32), value_float)
        mixed = mixed + scaling * jnp.einsum('the,hef->thf', query_dec.astype(jnp.float32), entering_float)
        inverse = lax.rsqrt(lax.optimization_barrier(jnp.mean(mixed * mixed, axis=2, keepdims=True)) + EPSILON)
        normed = mixed * inverse
        grad_normed = grad_block.astype(jnp.float32)
        grad_mixed = (inverse * (grad_normed - normed * lax.optimization_barrier(jnp.mean(grad_normed * normed, axis=2, keepdims=True)))).astype(jnp.bfloat16)
        grad_float = grad_mixed.astype(jnp.float32)
        back_state = scaling * jnp.einsum('the,thf->hef', query_dec.astype(jnp.float32), grad_float)
        leaving_float = later_state.astype(jnp.bfloat16).astype(jnp.float32)
        grad_prob = jnp.einsum('thf,shf->hts', grad_float, value_float)
        grad_score = (grad_prob * scaling * decay_mat).astype(jnp.bfloat16).astype(jnp.float32)
        grad_q = jnp.einsum('hts,she->the', grad_score, key_block.astype(jnp.float32))
        grad_q = grad_q + scaling * growth * jnp.einsum('thf,hef->the', grad_float, entering_float)
        grad_k = jnp.einsum('hts,the->she', grad_score, query_block.astype(jnp.float32))
        grad_k = grad_k + shrink * jnp.einsum('shf,hef->she', value_float, leaving_float)
        grad_v = jnp.einsum('hts,thf->shf', weights.astype(jnp.float32), grad_float)
        grad_v = grad_v + jnp.einsum('she,hef->shf', key_dec.astype(jnp.float32), leaving_float)
        new_later = jnp.exp(totals)[:, None, None] * later_state + back_state
        return (new_later, (normed.astype(jnp.bfloat16), grad_q.astype(jnp.bfloat16), grad_k.astype(jnp.bfloat16), grad_v.astype(jnp.bfloat16)))
    _, results = lax.scan(backward_step, start_state, (query_all, key_all, value_all, decay_all, entering, grad_all), reverse=True)
    attended, grad_queries, grad_keys, grad_values = [piece.reshape(SEQUENCE_TOKENS, HALF_HEADS * E) for piece in results]
    return (attended, grad_queries, grad_keys, grad_values)
```

```python
import functools
import math

import jax
import jax.numpy as jnp
from jax import lax
from jax.experimental import pallas as pl
from jax.experimental.pallas import tpu as pltpu
from jax.sharding import PartitionSpec as P

EPSILON = 1e-06
F32 = jnp.float32
BF16 = jnp.bfloat16
MESH = pl.DeviceIdType.MESH
UNITS = 4
UNROLL = 16
PACE = 5.6
READY = {"S": 3.6, "C": 7.0, "M": 10.8, "G": 12.3, "BS": 16.4, "BC": 19.8, "F": 23.6}


def dot(a, b, da, db):
    return lax.dot_general(a, b, (((da,), (db,)), ((), ())), preferred_element_type=F32)


def kernel(outer_size, inner_size, units, q_hbm, k_hbm, v_hbm, decay_hbm, g_hbm,
           att_ref, gq_ref, gk_ref, gv_ref,
           q_ref, k_ref, v_ref, decay_ref, g_ref,
           run_ref, col_ref, tot_ref, fac_ref, facs_ref, spread_ref, dec_ref, w_ref, kd_ref, mix_ref, gm_ref,
           send1, recv1, out1, ret1, agg1, send2, recv2, out2, ret2, agg2, ent_ref, gkl_ref, gvl_ref,
           load_sems, fac_sems, send_sems, recv_sems):
    n = outer_size * inner_size
    half_inner = inner_size // 2
    count = n // 2
    heads, tokens = decay_ref.shape
    size = q_ref.shape[1] // heads
    scaling = 1.0 / math.sqrt(size)
    per_unit = heads // units
    rows = per_unit * size // count
    lanes = size // heads
    place_o, place_i = lax.axis_index("outer"), lax.axis_index("inner")
    half = lax.div(place_i, half_inner)
    near = lax.rem(place_i, half_inner)
    seat = place_o * half_inner + near
    mine = lax.div(seat * rows, size)
    partner = (place_o, lax.rem(place_i + half_inner, inner_size))

    def unit_heads(u):
        return range(u * per_unit, (u + 1) * per_unit)

    def unit_span(u):
        return pl.ds(u * per_unit * size, per_unit * size)

    def span(h):
        return pl.ds(h * size, size)

    decay_load = pltpu.make_async_copy(decay_hbm, decay_ref, load_sems.at[0, 0])
    decay_load.start()
    loads = {}
    for at, (name, source, target) in enumerate(
            (("k", k_hbm, k_ref), ("v", v_hbm, v_ref), ("q", q_hbm, q_ref), ("g", g_hbm, g_ref))):
        for u in range(units):
            loads[name, u] = pltpu.make_async_copy(
                source.at[:, unit_span(u)], target.at[:, unit_span(u)], load_sems.at[at + 1, u])
    for u in range(units):
        loads["k", u].start()
        loads["v", u].start()

    shifts = [(do, di) for do in range(outer_size) for di in range(half_inner) if do or di]
    shifts.sort(key=lambda s: (s[1] % 2 == 0, s[0] % 2 == 0, s[0] == 0))
    far = [s for s in shifts if s[1] % 2]
    close = [s for s in shifts if not s[1] % 2]
    shifts = [s for pair in zip(far, close) for s in pair] + far[len(close):] + close[len(far):]

    def peers(act):
        def one(do, di):
            o = lax.rem(place_o + do, outer_size)
            i = lax.rem(near + di, half_inner)
            act(o, half * half_inner + i, o * half_inner + i)

        if count <= UNROLL:
            for do, di in shifts:
                one(do, di)
        else:
            def turn(step, carry):
                one(lax.rem(step + 1, outer_size), lax.div(step + 1, outer_size))
                return carry
            lax.fori_loop(0, count - 1, turn, 0)

    barrier = pltpu.get_barrier_semaphore()
    peers(lambda o, i, s: pl.semaphore_signal(barrier, inc=1, device_id=(o, i), device_id_type=MESH))
    pl.semaphore_signal(barrier, inc=1, device_id=partner, device_id_type=MESH)

    for name in ("q", "g"):
        for u in range(units):
            loads[name, u].start()

    def piece(buffer, u, s):
        return buffer.at[u, pl.ds(pl.multiple_of(s * rows, rows), rows)]

    def others(buffer, u):
        return buffer.at[u, pl.ds(0, (count - 1) * rows)]

    def exchange(source, target, phase, u):
        peers(lambda o, i, s: pltpu.make_async_remote_copy(
            src_ref=piece(source, u, s), dst_ref=piece(target, u, seat),
            send_sem=send_sems.at[phase, u], recv_sem=recv_sems.at[phase, u],
            device_id=(o, i), device_id_type=MESH).start())
        keep = pl.ds(pl.multiple_of(seat * rows, rows), rows)
        target[u, keep] = source[u, keep]

    def across(sums, phase, u):
        pltpu.make_async_remote_copy(
            src_ref=sums.at[u, half], dst_ref=sums.at[u, half],
            send_sem=send_sems.at[phase, u], recv_sem=recv_sems.at[phase, u],
            device_id=partner, device_id_type=MESH).start()

    def drain(piece, sem):
        pltpu.make_async_copy(piece, piece, sem).wait()

    decay_load.wait()
    running = decay_ref[...]
    lane = lax.broadcasted_iota(jnp.int32, (heads, tokens), 1)
    shift = 1
    while shift < tokens:
        running = running + jnp.where(lane >= shift, pltpu.roll(running, shift, 1), 0.0)
        shift *= 2
    run_ref[...] = running
    totals = jnp.broadcast_to(running[:, tokens - 1:], (heads, size))
    own = lax.broadcasted_iota(jnp.int32, (heads, size), 1) // lanes == lax.broadcasted_iota(jnp.int32, (heads, size), 0)
    fac_ref[...] = jnp.exp(jnp.sum(jnp.where(own, totals, 0.0), axis=0, keepdims=True))
    facs_ref[half, seat] = fac_ref[...]

    def state_of(u):
        loads["k", u].wait()
        loads["v", u].wait()
        for h in unit_heads(u):
            row = running[h:h + 1]
            column = jnp.broadcast_to(row, (size, tokens)).T
            col_ref[h] = column
            total = jnp.broadcast_to(row[:, tokens - 1:], (1, size))
            tot_ref[h] = total
            cols = span(h)
            key_dec = (k_ref[:, cols].astype(F32) * jnp.exp(total - column)).astype(BF16)
            kd_ref[:, cols] = key_dec
            send1[u, pl.ds((h - u * per_unit) * size, size)] = dot(key_dec, v_ref[:, cols], 0, 0)

    t_index = lax.broadcasted_iota(jnp.int32, (tokens, tokens), 0)
    s_index = lax.broadcasted_iota(jnp.int32, (tokens, tokens), 1)
    causal = s_index <= t_index

    def local_mix(u):
        loads["q", u].wait()
        for h in unit_heads(u):
            cols = span(h)
            column = jnp.concatenate([col_ref[h]] * (tokens // size), axis=1)
            gaps = column - run_ref[pl.ds(h, 1)]
            decay = jnp.where(causal, jnp.exp(jnp.where(causal, gaps, 0.0)), 0.0) * scaling
            dec_ref[h] = decay
            weights = (dot(q_ref[:, cols], k_ref[:, cols], 1, 1) * decay).astype(BF16)
            w_ref[h] = weights
            mix_ref[:, cols] = dot(weights, v_ref[:, cols], 1, 0)

    lane_of = lax.broadcasted_iota(jnp.int32, (count, size), 1)

    def spread(side):
        block = facs_ref[side].reshape(count, size)
        for u in range(units):
            one = jnp.sum(jnp.where(lane_of == (u * per_unit + mine) * lanes, block, 0.0), axis=1, keepdims=True)
            spread_ref[u, side] = jnp.broadcast_to(one, (count, size))

    def factor_of(u, side, s):
        return spread_ref[u, side, pl.ds(s, 1)]

    def fold(source, sums, u, phase, backward):
        drain(others(source, u), recv_sems.at[phase, u])
        for o in range(outer_size):
            state = None
            for step in range(half_inner):
                s = o * half_inner + (half_inner - 1 - step if backward else step)
                term = source[u, pl.ds(s * rows, rows)]
                state = term if state is None else factor_of(u, half, s) * state + term
            sums[u, half, o] = state
        across(sums, phase + 1, u)

    def scan(source, sums, target, result, u, phase, backward):
        drain(sums.at[u, 1 - half], recv_sems.at[phase + 1, u])
        order = (1, 0) if backward else (0, 1)
        carry = jnp.zeros((rows, size), F32)
        for turn in range(outer_size):
            o = outer_size - 1 - turn if backward else turn
            entry = []
            for side in order:
                entry.append(carry)
                factor = factor_of(u, side, o * half_inner)
                for step in range(1, half_inner):
                    factor = factor * factor_of(u, side, o * half_inner + step)
                carry = factor * carry + sums[u, side, o]
            state = jnp.where(half == order[0], entry[0], entry[1])
            for step in range(half_inner):
                s = o * half_inner + (half_inner - 1 - step if backward else step)
                target[u, pl.ds(s * rows, rows)] = state
                if step < half_inner - 1:
                    state = factor_of(u, half, s) * state + source[u, pl.ds(s * rows, rows)]
        exchange(target, result, phase + 2, u)

    def mix(u):
        drain(others(ret1, u), recv_sems.at[2, u])
        loads["g", u].wait()
        for h in unit_heads(u):
            cols = span(h)
            part = pl.ds((h - u * per_unit) * size, size)
            entering = ret1[u, part].astype(BF16)
            ent_ref[h] = entering
            growth = jnp.exp(col_ref[h])
            query_dec = (q_ref[:, cols].astype(F32) * growth).astype(BF16)
            mixed = mix_ref[:, cols] + scaling * dot(query_dec, entering, 1, 0)
            inverse = lax.rsqrt(jnp.mean(mixed * mixed, axis=1, keepdims=True) + EPSILON)
            normed = mixed * inverse
            att_ref[:, cols] = normed.astype(BF16)
            g = g_ref[:, cols].astype(F32)
            grad_mixed = (inverse * (g - normed * jnp.mean(g * normed, axis=1, keepdims=True))).astype(BF16)
            gm_ref[:, cols] = grad_mixed
            send2[u, part] = scaling * dot(query_dec, grad_mixed, 0, 0)
        exchange(send2, recv2, 3, u)

    def local_grads(u):
        for h in unit_heads(u):
            cols = span(h)
            grad_mixed = gm_ref[:, cols]
            grad_score = (dot(grad_mixed, v_ref[:, cols], 1, 1) * dec_ref[h]).astype(BF16)
            away = (scaling * jnp.exp(col_ref[h])) * dot(grad_mixed, ent_ref[h], 1, 1)
            gq_ref[:, cols] = (dot(grad_score, k_ref[:, cols], 1, 0) + away).astype(BF16)
            gkl_ref[:, cols] = dot(grad_score, q_ref[:, cols], 0, 0)
            gvl_ref[:, cols] = dot(w_ref[h], grad_mixed, 0, 0)

    def far_grads(u):
        drain(others(ret2, u), recv_sems.at[5, u])
        for h in unit_heads(u):
            cols = span(h)
            leaving = ret2[u, pl.ds((h - u * per_unit) * size, size)].astype(BF16)
            shrink = jnp.exp(tot_ref[h] - col_ref[h])
            gk_ref[:, cols] = (gkl_ref[:, cols] + shrink * dot(v_ref[:, cols], leaving, 1, 1)).astype(BF16)
            gv_ref[:, cols] = (gvl_ref[:, cols] + dot(kd_ref[:, cols], leaving, 1, 0)).astype(BF16)

    for u in range(units):
        state_of(u)
        if u == 0:
            pl.semaphore_wait(barrier, count)
        exchange(send1, recv1, 0, u)
        if u == 0:
            peers(lambda o, i, s: pltpu.make_async_remote_copy(
                src_ref=fac_ref, dst_ref=facs_ref.at[half, seat],
                send_sem=fac_sems.at[0], recv_sem=fac_sems.at[1],
                device_id=(o, i), device_id_type=MESH).start())
    for u in range(units):
        local_mix(u)
        if u == 0:
            drain(facs_ref.at[0, pl.ds(0, count - 1)], fac_sems.at[1])
            pltpu.make_async_remote_copy(
                src_ref=facs_ref.at[half], dst_ref=facs_ref.at[half],
                send_sem=fac_sems.at[2], recv_sem=fac_sems.at[3],
                device_id=partner, device_id_type=MESH).start()
            spread(half)

    def first_scan(u):
        if u == 0:
            drain(facs_ref.at[1 - half], fac_sems.at[3])
            spread(1 - half)
        scan(recv1, agg1, out1, ret1, u, 0, False)

    acts = {
        "S": lambda u: fold(recv1, agg1, u, 0, False),
        "C": first_scan,
        "M": mix,
        "G": local_grads,
        "BS": lambda u: fold(recv2, agg2, u, 3, True),
        "BC": lambda u: scan(recv2, agg2, out2, ret2, u, 3, True),
        "F": far_grads,
    }
    plan = sorted((READY[name] + PACE * u / units, name, u) for name in acts for u in range(units))
    for _, name, u in plan:
        acts[name](u)

    drain(facs_ref.at[0, pl.ds(0, count - 1)], fac_sems.at[0])
    drain(facs_ref.at[half], fac_sems.at[2])
    for u in range(units):
        for phase, buffer in ((0, send1), (2, out1), (3, send2), (5, out2)):
            drain(others(buffer, u), send_sems.at[phase, u])
        drain(agg1.at[u, half], send_sems.at[1, u])
        drain(agg2.at[u, half], send_sems.at[4, u])


def store(*refs):
    sources, targets, sems = refs[:4], refs[4:8], refs[8]
    copies = [pltpu.make_async_copy(s, t, sems.at[at]) for at, (s, t) in enumerate(zip(sources, targets))]
    for copy in copies:
        copy.start()
    for copy in copies:
        copy.wait()


def body(outer_size, inner_size, query_rows, key_rows, value_rows, log_decay, grad_out):
    n = outer_size * inner_size
    heads, tokens = log_decay.shape
    wide = query_rows.shape[1]
    size = wide // heads
    count = n // 2
    units = UNITS
    while units > 1 and (heads % units or (heads // units) * size % (8 * count)):
        units //= 2
    rows = heads // units * size // count
    pieces = pltpu.VMEM((units, count * rows, size), F32)
    sums = pltpu.VMEM((units, 2, outer_size, rows, size), F32)
    vmem = pl.BlockSpec(memory_space=pltpu.VMEM)
    hbm = pl.BlockSpec(memory_space=pltpu.HBM)
    row_block = pltpu.VMEM((tokens, wide), BF16)
    outs = [jax.ShapeDtypeStruct((tokens, wide), BF16)] * 4
    results = pl.pallas_call(
        functools.partial(kernel, outer_size, inner_size, units),
        out_shape=outs,
        in_specs=[hbm] * 5,
        out_specs=[vmem] * 4,
        scratch_shapes=[
            row_block, row_block, row_block, pltpu.VMEM((heads, tokens), F32), row_block,
            pltpu.VMEM((heads, tokens), F32),
            pltpu.VMEM((heads, tokens, size), F32),
            pltpu.VMEM((heads, 1, size), F32),
            pltpu.VMEM((1, size), F32),
            pltpu.VMEM((2, count, 1, size), F32),
            pltpu.VMEM((units, 2, count, size), F32),
            pltpu.VMEM((heads, tokens, tokens), F32),
            pltpu.VMEM((heads, tokens, tokens), BF16),
            row_block,
            pltpu.VMEM((tokens, wide), F32),
            row_block,
            pieces, pieces, pieces, pieces, sums, pieces, pieces, pieces, pieces, sums,
            pltpu.VMEM((heads, size, size), BF16),
            pltpu.VMEM((tokens, wide), F32),
            pltpu.VMEM((tokens, wide), F32),
            pltpu.SemaphoreType.DMA((5, units)),
            pltpu.SemaphoreType.DMA((4,)),
            pltpu.SemaphoreType.DMA((6, units)),
            pltpu.SemaphoreType.DMA((6, units)),
        ],
        compiler_params=pltpu.CompilerParams(
            collective_id=0, has_side_effects=True, vmem_limit_bytes=40 * 1024 * 1024),
    )(*[pltpu.with_memory_space_constraint(x, pltpu.HBM) for x in (query_rows, key_rows, value_rows, log_decay, grad_out)])
    return pl.pallas_call(
        store,
        out_shape=outs,
        in_specs=[vmem] * 4,
        out_specs=[hbm] * 4,
        scratch_shapes=[pltpu.SemaphoreType.DMA((4,))],
        compiler_params=pltpu.CompilerParams(vmem_limit_bytes=8 * 1024 * 1024),
    )(*results)


def solution(mesh):
    both = ("outer", "inner")
    row_spec = P(both, None)
    return jax.shard_map(
        functools.partial(body, mesh.shape["outer"], mesh.shape["inner"]),
        mesh=mesh,
        in_specs=(row_spec, row_spec, row_spec, P(None, both), row_spec),
        out_specs=(row_spec,) * 4,
        check_vma=False,
    )
```

```python
import functools
import math

import jax
import jax.numpy as jnp
from jax import lax
from jax.experimental import pallas as pl
from jax.experimental.pallas import tpu as pltpu
from jax.sharding import PartitionSpec as P

EPSILON = 1e-06
F32 = jnp.float32
BF16 = jnp.bfloat16
MESH = pl.DeviceIdType.MESH
SHARES = (2, 2, 2, 2)
UNROLL = 16


def plan(units):
    every = range(units)
    steps = [("A", 0), ("b", 0), ("f", 0), ("X", 0)]
    for u in range(1, units):
        steps += [("A", u), ("X", u)]
    steps += [("L", u) for u in every] + [("r", 0)]
    steps += [("S", u) for u in every] + [("C", u) for u in every]
    for u in every:
        steps += [("M", u), ("Y", u), ("G", u)]
    steps += [(act, u) for act in "VWZ" for u in every]
    return steps


def dot(a, b, da, db):
    return lax.dot_general(a, b, (((da,), (db,)), ((), ())), preferred_element_type=F32)


def kernel(outer_size, inner_size, shares, q_hbm, k_hbm, v_hbm, decay_hbm, g_hbm,
           att_ref, gq_ref, gk_ref, gv_ref,
           q_ref, k_ref, v_ref, decay_ref, g_ref,
           run_ref, col_ref, tot_ref, fac_ref, facs_ref, spread_ref, dec_ref, w_ref, kd_ref, mix_ref, gm_ref,
           send1, recv1, out1, ret1, agg1, send2, recv2, out2, ret2, agg2, ent_ref, gkl_ref, gvl_ref,
           load_sems, fac_sems, send_sems, recv_sems):
    n = outer_size * inner_size
    half_inner = inner_size // 2
    extra = (outer_size + 7) // 8 * 8
    count = n // 2
    heads, tokens = decay_ref.shape
    size = q_ref.shape[1] // heads
    scaling = 1.0 / math.sqrt(size)
    units = len(shares)
    first = [sum(shares[:u]) for u in range(units)]
    rows = [share * size // count for share in shares]
    lanes = size // heads
    place_o, place_i = lax.axis_index("outer"), lax.axis_index("inner")
    half = lax.div(place_i, half_inner)
    near = lax.rem(place_i, half_inner)
    seat = place_o * half_inner + near
    partner = (place_o, lax.rem(place_i + half_inner, inner_size))

    def unit_heads(u):
        return range(first[u], first[u] + shares[u])

    def unit_span(u):
        return pl.ds(first[u] * size, shares[u] * size)

    def span(h):
        return pl.ds(h * size, size)

    decay_load = pltpu.make_async_copy(decay_hbm, decay_ref, load_sems.at[0, 0])
    decay_load.start()
    loads = {}
    for at, (name, source, target) in enumerate(
            (("k", k_hbm, k_ref), ("v", v_hbm, v_ref), ("q", q_hbm, q_ref), ("g", g_hbm, g_ref))):
        for u in range(units):
            loads[name, u] = pltpu.make_async_copy(
                source.at[:, unit_span(u)], target.at[:, unit_span(u)], load_sems.at[at + 1, u])
    for u in range(units):
        loads["k", u].start()
        loads["v", u].start()

    shifts = [(do, di) for do in range(outer_size) for di in range(half_inner) if do or di]
    far = [s for s in shifts if s[1] % 2]
    close = [s for s in shifts if not s[1] % 2]
    shifts = [s for pair in zip(far, close) for s in pair] + far[len(close):] + close[len(far):]

    def peers(act):
        def one(do, di):
            o = lax.rem(place_o + do, outer_size)
            i = lax.rem(near + di, half_inner)
            act(o, half * half_inner + i, o * half_inner + i)

        if count <= UNROLL:
            for do, di in shifts:
                one(do, di)
        else:
            def turn(step, carry):
                one(lax.rem(step + 1, outer_size), lax.div(step + 1, outer_size))
                return carry
            lax.fori_loop(0, count - 1, turn, 0)

    barrier = pltpu.get_barrier_semaphore()
    peers(lambda o, i, s: pl.semaphore_signal(barrier, inc=1, device_id=(o, i), device_id_type=MESH))
    pl.semaphore_signal(barrier, inc=1, device_id=partner, device_id_type=MESH)

    for name in ("q", "g"):
        for u in range(units):
            loads[name, u].start()

    def seat_rows(u, s):
        return pl.ds(pl.multiple_of(first[u] * size + s * rows[u], 8), rows[u])

    def others(buffer, u):
        return buffer.at[pl.ds(first[u] * size, (count - 1) * rows[u])]

    def exchange(source, target, phase, u):
        peers(lambda o, i, s: pltpu.make_async_remote_copy(
            src_ref=source.at[seat_rows(u, s)], dst_ref=target.at[seat_rows(u, seat)],
            send_sem=send_sems.at[phase, u], recv_sem=recv_sems.at[phase, u],
            device_id=(o, i), device_id_type=MESH).start())
        target[seat_rows(u, seat)] = source[seat_rows(u, seat)]

    starts = [outer_size * sum(rows[:u]) + extra * u for u in range(units)]
    plain = [outer_size * sum(rows[:u]) for u in range(units)]

    def side_sums(sums, side, u):
        if sums is agg1:
            return sums.at[side, pl.ds(starts[u], outer_size * rows[u] + extra)]
        return sums.at[side, pl.ds(plain[u], outer_size * rows[u])]

    def across(sums, phase, u):
        pltpu.make_async_remote_copy(
            src_ref=side_sums(sums, half, u), dst_ref=side_sums(sums, half, u),
            send_sem=send_sems.at[phase, u], recv_sem=recv_sems.at[phase, u],
            device_id=partner, device_id_type=MESH).start()

    def drain(piece, sem):
        pltpu.make_async_copy(piece, piece, sem).wait()

    decay_load.wait()
    running = decay_ref[...]
    lane = lax.broadcasted_iota(jnp.int32, (heads, tokens), 1)
    shift = 1
    while shift < tokens:
        running = running + jnp.where(lane >= shift, pltpu.roll(running, shift, 1), 0.0)
        shift *= 2
    run_ref[...] = running
    totals = jnp.broadcast_to(running[:, tokens - 1:], (heads, size))
    own = lax.broadcasted_iota(jnp.int32, (heads, size), 1) // lanes == lax.broadcasted_iota(jnp.int32, (heads, size), 0)
    fac_ref[...] = jnp.exp(jnp.sum(jnp.where(own, totals, 0.0), axis=0, keepdims=True))
    facs_ref[seat] = fac_ref[...]

    def state_of(u):
        loads["k", u].wait()
        loads["v", u].wait()
        for h in unit_heads(u):
            row = running[h:h + 1]
            column = jnp.broadcast_to(row, (size, tokens)).T
            col_ref[h] = column
            total = jnp.broadcast_to(row[:, tokens - 1:], (1, size))
            tot_ref[h] = total
            cols = span(h)
            key_dec = (k_ref[:, cols].astype(F32) * jnp.exp(total - column)).astype(BF16)
            kd_ref[:, cols] = key_dec
            send1[pl.ds(h * size, size)] = dot(key_dec, v_ref[:, cols], 0, 0)

    t_index = lax.broadcasted_iota(jnp.int32, (tokens, tokens), 0)
    s_index = lax.broadcasted_iota(jnp.int32, (tokens, tokens), 1)
    causal = s_index <= t_index

    def local_mix(u):
        loads["q", u].wait()
        for h in unit_heads(u):
            cols = span(h)
            column = jnp.concatenate([col_ref[h]] * (tokens // size), axis=1)
            gaps = column - run_ref[pl.ds(h, 1)]
            decay = jnp.where(causal, jnp.exp(jnp.where(causal, gaps, 0.0)), 0.0) * scaling
            dec_ref[h] = decay
            weights = (dot(q_ref[:, cols], k_ref[:, cols], 1, 1) * decay).astype(BF16)
            w_ref[h] = weights
            mix_ref[:, cols] = dot(weights, v_ref[:, cols], 1, 0)

    lane_of = lax.broadcasted_iota(jnp.int32, (count, size), 1)

    def spread():
        block = facs_ref[...].reshape(count, size)
        for u in range(units):
            one = jnp.sum(jnp.where(lane_of == (first[u] + lax.div(seat * rows[u], size)) * lanes, block, 0.0), axis=1, keepdims=True)
            spread_ref[u] = jnp.broadcast_to(one, (count, size))

    def factor_of(u, s):
        return spread_ref[u, pl.ds(s, 1)]

    def group_rows(sums, u, o):
        return pl.ds((starts if sums is agg1 else plain)[u] + o * rows[u], rows[u])

    def product_row(u, o):
        return pl.ds(starts[u] + outer_size * rows[u] + o, 1)

    def fold(source, sums, u, phase, backward):
        drain(others(source, u), recv_sems.at[phase, u])
        for o in range(outer_size):
            state = None
            for step in range(half_inner):
                s = o * half_inner + (half_inner - 1 - step if backward else step)
                term = source[seat_rows(u, s)]
                state = term if state is None else factor_of(u, s) * state + term
            sums[half, group_rows(sums, u, o)] = state
            if not backward:
                factor = factor_of(u, o * half_inner)
                for step in range(1, half_inner):
                    factor = factor * factor_of(u, o * half_inner + step)
                sums[half, product_row(u, o)] = factor
        across(sums, phase + 1, u)

    def scan(source, sums, target, result, u, phase, backward):
        drain(side_sums(sums, 1 - half, u), recv_sems.at[phase + 1, u])
        order = (1, 0) if backward else (0, 1)
        carry = jnp.zeros((rows[u], size), F32)
        for turn in range(outer_size):
            o = outer_size - 1 - turn if backward else turn
            entry = []
            for side in order:
                entry.append(carry)
                carry = agg1[side, product_row(u, o)] * carry + sums[side, group_rows(sums, u, o)]
            state = jnp.where(half == order[0], entry[0], entry[1])
            for step in range(half_inner):
                s = o * half_inner + (half_inner - 1 - step if backward else step)
                target[seat_rows(u, s)] = state
                if step < half_inner - 1:
                    state = factor_of(u, s) * state + source[seat_rows(u, s)]
        exchange(target, result, phase + 2, u)

    def mix(u):
        drain(others(ret1, u), recv_sems.at[2, u])
        loads["g", u].wait()
        for h in unit_heads(u):
            cols = span(h)
            part = pl.ds(h * size, size)
            entering = ret1[part].astype(BF16)
            ent_ref[h] = entering
            growth = jnp.exp(col_ref[h])
            query_dec = (q_ref[:, cols].astype(F32) * growth).astype(BF16)
            mixed = mix_ref[:, cols] + scaling * dot(query_dec, entering, 1, 0)
            inverse = lax.rsqrt(jnp.mean(mixed * mixed, axis=1, keepdims=True) + EPSILON)
            normed = mixed * inverse
            att_ref[:, cols] = normed.astype(BF16)
            g = g_ref[:, cols].astype(F32)
            grad_mixed = (inverse * (g - normed * jnp.mean(g * normed, axis=1, keepdims=True))).astype(BF16)
            gm_ref[:, cols] = grad_mixed
            send2[part] = scaling * dot(query_dec, grad_mixed, 0, 0)

    def local_grads(u):
        for h in unit_heads(u):
            cols = span(h)
            grad_mixed = gm_ref[:, cols]
            grad_score = (dot(grad_mixed, v_ref[:, cols], 1, 1) * dec_ref[h]).astype(BF16)
            away = (scaling * jnp.exp(col_ref[h])) * dot(grad_mixed, ent_ref[h], 1, 1)
            gq_ref[:, cols] = (dot(grad_score, k_ref[:, cols], 1, 0) + away).astype(BF16)
            gkl_ref[:, cols] = dot(grad_score, q_ref[:, cols], 0, 0)
            gvl_ref[:, cols] = dot(w_ref[h], grad_mixed, 0, 0)

    def far_grads(u):
        drain(others(ret2, u), recv_sems.at[5, u])
        for h in unit_heads(u):
            cols = span(h)
            leaving = ret2[pl.ds(h * size, size)].astype(BF16)
            shrink = jnp.exp(tot_ref[h] - col_ref[h])
            gk_ref[:, cols] = (gkl_ref[:, cols] + shrink * dot(v_ref[:, cols], leaving, 1, 1)).astype(BF16)
            gv_ref[:, cols] = (gvl_ref[:, cols] + dot(kd_ref[:, cols], leaving, 1, 0)).astype(BF16)

    def send_factors():
        peers(lambda o, i, s: pltpu.make_async_remote_copy(
            src_ref=fac_ref, dst_ref=facs_ref.at[seat],
            send_sem=fac_sems.at[0], recv_sem=fac_sems.at[1],
            device_id=(o, i), device_id_type=MESH).start())

    def take_factors():
        drain(facs_ref.at[pl.ds(0, count - 1)], fac_sems.at[1])
        spread()

    acts = {
        "b": lambda u: pl.semaphore_wait(barrier, count),
        "f": lambda u: send_factors(),
        "r": lambda u: take_factors(),
        "A": state_of,
        "X": lambda u: exchange(send1, recv1, 0, u),
        "L": local_mix,
        "S": lambda u: fold(recv1, agg1, u, 0, False),
        "C": lambda u: scan(recv1, agg1, out1, ret1, u, 0, False),
        "M": mix,
        "Y": lambda u: exchange(send2, recv2, 3, u),
        "G": local_grads,
        "V": lambda u: fold(recv2, agg2, u, 3, True),
        "W": lambda u: scan(recv2, agg2, out2, ret2, u, 3, True),
        "Z": far_grads,
    }
    for act, u in plan(units):
        acts[act](u)

    drain(facs_ref.at[pl.ds(0, count - 1)], fac_sems.at[0])
    for u in range(units):
        for phase, buffer in ((0, send1), (2, out1), (3, send2), (5, out2)):
            drain(others(buffer, u), send_sems.at[phase, u])
        drain(side_sums(agg1, half, u), send_sems.at[1, u])
        drain(side_sums(agg2, half, u), send_sems.at[4, u])


def store(*refs):
    sources, targets, sems = refs[:4], refs[4:8], refs[8]
    copies = [pltpu.make_async_copy(s, t, sems.at[at]) for at, (s, t) in enumerate(zip(sources, targets))]
    for copy in copies:
        copy.start()
    for copy in copies:
        copy.wait()


def body(outer_size, inner_size, query_rows, key_rows, value_rows, log_decay, grad_out):
    n = outer_size * inner_size
    heads, tokens = log_decay.shape
    wide = query_rows.shape[1]
    size = wide // heads
    count = n // 2
    shares = SHARES
    if sum(shares) != heads or any(share * size % (8 * count) for share in shares):
        shares = (heads,)
    units = len(shares)
    extra = (outer_size + 7) // 8 * 8
    pieces = pltpu.VMEM((heads * size, size), F32)
    sums = pltpu.VMEM((2, outer_size * heads * size // count, size), F32)
    summed = pltpu.VMEM((2, outer_size * heads * size // count + extra * units, size), F32)
    vmem = pl.BlockSpec(memory_space=pltpu.VMEM)
    hbm = pl.BlockSpec(memory_space=pltpu.HBM)
    row_block = pltpu.VMEM((tokens, wide), BF16)
    outs = [jax.ShapeDtypeStruct((tokens, wide), BF16)] * 4
    results = pl.pallas_call(
        functools.partial(kernel, outer_size, inner_size, shares),
        out_shape=outs,
        in_specs=[hbm] * 5,
        out_specs=[vmem] * 4,
        scratch_shapes=[
            row_block, row_block, row_block, pltpu.VMEM((heads, tokens), F32), row_block,
            pltpu.VMEM((heads, tokens), F32),
            pltpu.VMEM((heads, tokens, size), F32),
            pltpu.VMEM((heads, 1, size), F32),
            pltpu.VMEM((1, size), F32),
            pltpu.VMEM((count, 1, size), F32),
            pltpu.VMEM((units, count, size), F32),
            pltpu.VMEM((heads, tokens, tokens), F32),
            pltpu.VMEM((heads, tokens, tokens), BF16),
            row_block,
            pltpu.VMEM((tokens, wide), F32),
            row_block,
            pieces, pieces, pieces, pieces, summed, pieces, pieces, pieces, pieces, sums,
            pltpu.VMEM((heads, size, size), BF16),
            pltpu.VMEM((tokens, wide), F32),
            pltpu.VMEM((tokens, wide), F32),
            pltpu.SemaphoreType.DMA((5, units)),
            pltpu.SemaphoreType.DMA((2,)),
            pltpu.SemaphoreType.DMA((6, units)),
            pltpu.SemaphoreType.DMA((6, units)),
        ],
        compiler_params=pltpu.CompilerParams(
            collective_id=0, has_side_effects=True, vmem_limit_bytes=40 * 1024 * 1024),
    )(*[pltpu.with_memory_space_constraint(x, pltpu.HBM) for x in (query_rows, key_rows, value_rows, log_decay, grad_out)])
    return pl.pallas_call(
        store,
        out_shape=outs,
        in_specs=[vmem] * 4,
        out_specs=[hbm] * 4,
        scratch_shapes=[pltpu.SemaphoreType.DMA((4,))],
        compiler_params=pltpu.CompilerParams(vmem_limit_bytes=8 * 1024 * 1024),
    )(*results)


def solution(mesh):
    both = ("outer", "inner")
    row_spec = P(both, None)
    return jax.shard_map(
        functools.partial(body, mesh.shape["outer"], mesh.shape["inner"]),
        mesh=mesh,
        in_specs=(row_spec, row_spec, row_spec, P(None, both), row_spec),
        out_specs=(row_spec,) * 4,
        check_vma=False,
    )
```

```python
import functools
import math

import jax
import jax.numpy as jnp
from jax import lax
from jax.experimental import pallas as pl
from jax.experimental.pallas import tpu as pltpu
from jax.sharding import PartitionSpec as P

EPSILON = 1e-06
F32 = jnp.float32
BF16 = jnp.bfloat16
MESH = pl.DeviceIdType.MESH
SHARES = (2, 2, 2, 2)
UNROLL = 16
ORDER = lambda m: (-(m[1] % 2), -(m[1] // 2), -(m[0] % 2), -(m[0] // 2))


def plan(units):
    every = range(units)
    steps = [("A", 0), ("b", 0), ("f", 0), ("X", 0)]
    for u in range(1, units):
        steps += [("A", u), ("X", u)]
    steps += [("L", u) for u in every] + [("r", 0)]
    steps += [("S", u) for u in every] + [("t", 0)] + [("C", u) for u in every]
    for u in every:
        steps += [("M", u), ("Y", u), ("G", u)]
    steps += [(act, u) for act in "VWZ" for u in every]
    return steps


def dot(a, b, da, db):
    return lax.dot_general(a, b, (((da,), (db,)), ((), ())), preferred_element_type=F32)


def kernel(outer_size, inner_size, shares, q_hbm, k_hbm, v_hbm, decay_hbm, g_hbm,
           att_ref, gq_ref, gk_ref, gv_ref,
           q_ref, k_ref, v_ref, decay_ref, g_ref,
           run_ref, col_ref, shrink_ref, qd_ref, fac_ref, facs_ref, spread_ref, prod_ref, whole_ref, dec_ref, w_ref, kd_ref, mix_ref, gm_ref,
           send1, recv1, out1, ret1, agg1, send2, recv2, out2, ret2, agg2, ent_ref, gkl_ref, gvl_ref,
           load_sems, fac_sems, send_sems, recv_sems):
    n = outer_size * inner_size
    half_inner = inner_size // 2
    count = n // 2
    heads, tokens = decay_ref.shape
    size = q_ref.shape[1] // heads
    scaling = 1.0 / math.sqrt(size)
    units = len(shares)
    first = [sum(shares[:u]) for u in range(units)]
    rows = [share * size // count for share in shares]
    lanes = size // heads
    place_o, place_i = lax.axis_index("outer"), lax.axis_index("inner")
    half = lax.div(place_i, half_inner)
    near = lax.rem(place_i, half_inner)
    seat = place_o * half_inner + near
    partner = (place_o, lax.rem(place_i + half_inner, inner_size))

    def unit_heads(u):
        return range(first[u], first[u] + shares[u])

    def unit_span(u):
        return pl.ds(first[u] * size, shares[u] * size)

    def span(h):
        return pl.ds(h * size, size)

    decay_load = pltpu.make_async_copy(decay_hbm, decay_ref, load_sems.at[0, 0])
    decay_load.start()
    loads = {}
    for at, (name, source, target) in enumerate(
            (("k", k_hbm, k_ref), ("v", v_hbm, v_ref), ("q", q_hbm, q_ref), ("g", g_hbm, g_ref))):
        for u in range(units):
            loads[name, u] = pltpu.make_async_copy(
                source.at[:, unit_span(u)], target.at[:, unit_span(u)], load_sems.at[at + 1, u])
    for u in range(units):
        loads["k", u].start()
        loads["v", u].start()

    def flipped(place, mask):
        bit = 1
        while bit <= mask:
            if mask & bit:
                place = place + bit * (1 - 2 * lax.rem(lax.div(place, bit), 2))
            bit *= 2
        return place

    binary = outer_size & (outer_size - 1) == 0 and half_inner & (half_inner - 1) == 0
    masks = [(mo, mi) for mo in range(outer_size) for mi in range(half_inner) if mo or mi]
    masks.sort(key=ORDER)

    def peers(act):
        def one(o, i):
            act(o, half * half_inner + i, o * half_inner + i)

        if binary and count <= UNROLL:
            for mo, mi in masks:
                one(flipped(place_o, mo), flipped(near, mi))
        else:
            def turn(step, carry):
                one(lax.rem(place_o + lax.rem(step + 1, outer_size), outer_size),
                    lax.rem(near + lax.div(step + 1, outer_size), half_inner))
                return carry
            lax.fori_loop(0, count - 1, turn, 0)

    barrier = pltpu.get_barrier_semaphore()
    peers(lambda o, i, s: pl.semaphore_signal(barrier, inc=1, device_id=(o, i), device_id_type=MESH))
    pl.semaphore_signal(barrier, inc=1, device_id=partner, device_id_type=MESH)

    for name in ("q", "g"):
        for u in range(units):
            loads[name, u].start()

    def seat_rows(u, s):
        return pl.ds(pl.multiple_of(first[u] * size + s * rows[u], 8), rows[u])

    def others(buffer, u):
        return buffer.at[pl.ds(first[u] * size, (count - 1) * rows[u])]

    def exchange(source, target, phase, u):
        peers(lambda o, i, s: pltpu.make_async_remote_copy(
            src_ref=source.at[seat_rows(u, s)], dst_ref=target.at[seat_rows(u, seat)],
            send_sem=send_sems.at[phase, u], recv_sem=recv_sems.at[phase, u],
            device_id=(o, i), device_id_type=MESH).start())
        target[seat_rows(u, seat)] = source[seat_rows(u, seat)]

    plain = [outer_size * sum(rows[:u]) for u in range(units)]

    def side_sums(sums, side, u):
        return sums.at[side, pl.ds(plain[u], outer_size * rows[u])]

    def across(sums, phase, u):
        pltpu.make_async_remote_copy(
            src_ref=side_sums(sums, half, u), dst_ref=side_sums(sums, half, u),
            send_sem=send_sems.at[phase, u], recv_sem=recv_sems.at[phase, u],
            device_id=partner, device_id_type=MESH).start()

    def drain(piece, sem):
        pltpu.make_async_copy(piece, piece, sem).wait()

    decay_load.wait()
    running = decay_ref[...]
    lane = lax.broadcasted_iota(jnp.int32, (heads, tokens), 1)
    shift = 1
    while shift < tokens:
        running = running + jnp.where(lane >= shift, pltpu.roll(running, shift, 1), 0.0)
        shift *= 2
    run_ref[...] = running
    totals = jnp.broadcast_to(running[:, tokens - 1:], (heads, size))
    own = lax.broadcasted_iota(jnp.int32, (heads, size), 1) // lanes == lax.broadcasted_iota(jnp.int32, (heads, size), 0)
    fac_ref[...] = jnp.exp(jnp.sum(jnp.where(own, totals, 0.0), axis=0, keepdims=True))
    facs_ref[seat] = fac_ref[...]

    def state_of(u):
        loads["k", u].wait()
        loads["v", u].wait()
        for h in unit_heads(u):
            row = running[h:h + 1]
            column = jnp.broadcast_to(row, (size, tokens)).T
            col_ref[h] = column
            total = jnp.broadcast_to(row[:, tokens - 1:], (1, size))
            cols = span(h)
            shrink = jnp.exp(total - column)
            shrink_ref[h] = shrink
            key_dec = (k_ref[:, cols].astype(F32) * shrink).astype(BF16)
            kd_ref[:, cols] = key_dec
            send1[pl.ds(h * size, size)] = dot(key_dec, v_ref[:, cols], 0, 0)

    t_index = lax.broadcasted_iota(jnp.int32, (tokens, tokens), 0)
    s_index = lax.broadcasted_iota(jnp.int32, (tokens, tokens), 1)
    causal = s_index <= t_index

    def local_mix(u):
        loads["q", u].wait()
        for h in unit_heads(u):
            cols = span(h)
            column = jnp.concatenate([col_ref[h]] * (tokens // size), axis=1)
            gaps = column - run_ref[pl.ds(h, 1)]
            decay = jnp.where(causal, jnp.exp(jnp.where(causal, gaps, 0.0)), 0.0) * scaling
            dec_ref[h] = decay
            weights = (dot(q_ref[:, cols], k_ref[:, cols], 1, 1) * decay).astype(BF16)
            w_ref[h] = weights
            mix_ref[:, cols] = dot(weights, v_ref[:, cols], 1, 0)
            qd_ref[:, cols] = (q_ref[:, cols].astype(F32) * jnp.exp(col_ref[h])).astype(BF16)

    lane_of = lax.broadcasted_iota(jnp.int32, (count, size), 1)

    def spread():
        block = facs_ref[...].reshape(count, size)
        for u in range(units):
            one = jnp.sum(jnp.where(lane_of == (first[u] + lax.div(seat * rows[u], size)) * lanes, block, 0.0), axis=1, keepdims=True)
            spread_ref[u] = jnp.broadcast_to(one, (count, size))

    def spread_products(side):
        block = prod_ref[side]
        lane_at = lax.broadcasted_iota(jnp.int32, block.shape, 1)
        for u in range(units):
            head = first[u] + lax.div(seat * rows[u], size)
            one = jnp.sum(jnp.where(lane_at == head * lanes, block, 0.0), axis=1, keepdims=True)
            whole_ref[u, side] = jnp.broadcast_to(one, block.shape)

    def factor_of(u, s):
        return spread_ref[u, pl.ds(s, 1)]

    def group_rows(sums, u, o):
        return pl.ds(plain[u] + o * rows[u], rows[u])

    def fold(source, sums, u, phase, backward):
        drain(others(source, u), recv_sems.at[phase, u])
        for o in range(outer_size):
            state = None
            for step in range(half_inner):
                s = o * half_inner + (half_inner - 1 - step if backward else step)
                term = source[seat_rows(u, s)]
                state = term if state is None else factor_of(u, s) * state + term
            sums[half, group_rows(sums, u, o)] = state
        across(sums, phase + 1, u)

    def scan(source, sums, target, result, u, phase, backward):
        drain(side_sums(sums, 1 - half, u), recv_sems.at[phase + 1, u])
        order = (1, 0) if backward else (0, 1)
        carry = jnp.zeros((rows[u], size), F32)
        for turn in range(outer_size):
            o = outer_size - 1 - turn if backward else turn
            entry = []
            for side in order:
                entry.append(carry)
                carry = whole_ref[u, side, pl.ds(o, 1)] * carry + sums[side, group_rows(sums, u, o)]
            state = jnp.where(half == order[0], entry[0], entry[1])
            for step in range(half_inner):
                s = o * half_inner + (half_inner - 1 - step if backward else step)
                target[seat_rows(u, s)] = state
                if step < half_inner - 1:
                    state = factor_of(u, s) * state + source[seat_rows(u, s)]
        exchange(target, result, phase + 2, u)

    def mix(u):
        drain(others(ret1, u), recv_sems.at[2, u])
        loads["g", u].wait()
        for h in unit_heads(u):
            cols = span(h)
            part = pl.ds(h * size, size)
            entering = ret1[part].astype(BF16)
            ent_ref[h] = entering
            query_dec = qd_ref[:, cols]
            mixed = mix_ref[:, cols] + scaling * dot(query_dec, entering, 1, 0)
            inverse = lax.rsqrt(jnp.mean(mixed * mixed, axis=1, keepdims=True) + EPSILON)
            normed = mixed * inverse
            att_ref[:, cols] = normed.astype(BF16)
            g = g_ref[:, cols].astype(F32)
            grad_mixed = (inverse * (g - normed * jnp.mean(g * normed, axis=1, keepdims=True))).astype(BF16)
            gm_ref[:, cols] = grad_mixed
            send2[part] = scaling * dot(query_dec, grad_mixed, 0, 0)

    def local_grads(u):
        for h in unit_heads(u):
            cols = span(h)
            grad_mixed = gm_ref[:, cols]
            grad_score = (dot(grad_mixed, v_ref[:, cols], 1, 1) * dec_ref[h]).astype(BF16)
            away = (scaling * jnp.exp(col_ref[h])) * dot(grad_mixed, ent_ref[h], 1, 1)
            gq_ref[:, cols] = (dot(grad_score, k_ref[:, cols], 1, 0) + away).astype(BF16)
            gkl_ref[:, cols] = dot(grad_score, q_ref[:, cols], 0, 0)
            gvl_ref[:, cols] = dot(w_ref[h], grad_mixed, 0, 0)

    def far_grads(u):
        drain(others(ret2, u), recv_sems.at[5, u])
        for h in unit_heads(u):
            cols = span(h)
            leaving = ret2[pl.ds(h * size, size)].astype(BF16)
            gk_ref[:, cols] = (gkl_ref[:, cols] + shrink_ref[h] * dot(v_ref[:, cols], leaving, 1, 1)).astype(BF16)
            gv_ref[:, cols] = (gvl_ref[:, cols] + dot(kd_ref[:, cols], leaving, 1, 0)).astype(BF16)

    def send_factors():
        peers(lambda o, i, s: pltpu.make_async_remote_copy(
            src_ref=fac_ref, dst_ref=facs_ref.at[seat],
            send_sem=fac_sems.at[0], recv_sem=fac_sems.at[1],
            device_id=(o, i), device_id_type=MESH).start())

    def take_factors():
        drain(facs_ref.at[pl.ds(0, count - 1)], fac_sems.at[1])
        prod_ref[half] = jnp.zeros(prod_ref.shape[1:], F32)
        for o in range(outer_size):
            product = facs_ref[o * half_inner]
            for step in range(1, half_inner):
                product = product * facs_ref[o * half_inner + step]
            prod_ref[half, pl.ds(o, 1)] = product
        pltpu.make_async_remote_copy(
            src_ref=prod_ref.at[half], dst_ref=prod_ref.at[half],
            send_sem=fac_sems.at[2], recv_sem=fac_sems.at[3],
            device_id=partner, device_id_type=MESH).start()
        spread()
        spread_products(half)

    def take_products():
        drain(prod_ref.at[1 - half], fac_sems.at[3])
        spread_products(1 - half)

    acts = {
        "b": lambda u: pl.semaphore_wait(barrier, count),
        "f": lambda u: send_factors(),
        "r": lambda u: take_factors(),
        "t": lambda u: take_products(),
        "A": state_of,
        "X": lambda u: exchange(send1, recv1, 0, u),
        "L": local_mix,
        "S": lambda u: fold(recv1, agg1, u, 0, False),
        "C": lambda u: scan(recv1, agg1, out1, ret1, u, 0, False),
        "M": mix,
        "Y": lambda u: exchange(send2, recv2, 3, u),
        "G": local_grads,
        "V": lambda u: fold(recv2, agg2, u, 3, True),
        "W": lambda u: scan(recv2, agg2, out2, ret2, u, 3, True),
        "Z": far_grads,
    }
    for act, u in plan(units):
        acts[act](u)

    drain(facs_ref.at[pl.ds(0, count - 1)], fac_sems.at[0])
    drain(prod_ref.at[half], fac_sems.at[2])
    for u in range(units):
        for phase, buffer in ((0, send1), (2, out1), (3, send2), (5, out2)):
            drain(others(buffer, u), send_sems.at[phase, u])
        drain(side_sums(agg1, half, u), send_sems.at[1, u])
        drain(side_sums(agg2, half, u), send_sems.at[4, u])


def store(*refs):
    sources, targets, sems = refs[:4], refs[4:8], refs[8]
    tokens = sources[0].shape[0]
    cut = tokens // 1
    copies = [pltpu.make_async_copy(s.at[pl.ds(c * cut, cut)], t.at[pl.ds(c * cut, cut)], sems.at[at, c])
              for c in range(1) for at, (s, t) in enumerate(zip(sources, targets))]
    for copy in copies:
        copy.start()
    for copy in copies:
        copy.wait()


def body(outer_size, inner_size, query_rows, key_rows, value_rows, log_decay, grad_out):
    n = outer_size * inner_size
    heads, tokens = log_decay.shape
    wide = query_rows.shape[1]
    size = wide // heads
    count = n // 2
    shares = SHARES
    if sum(shares) != heads or any(share * size % (8 * count) for share in shares):
        shares = (heads,)
    units = len(shares)
    extra = (outer_size + 7) // 8 * 8
    pieces = pltpu.VMEM((heads * size, size), F32)
    sums = pltpu.VMEM((2, outer_size * heads * size // count, size), F32)
    vmem = pl.BlockSpec(memory_space=pltpu.VMEM)
    hbm = pl.BlockSpec(memory_space=pltpu.HBM)
    row_block = pltpu.VMEM((tokens, wide), BF16)
    outs = [jax.ShapeDtypeStruct((tokens, wide), BF16)] * 4
    results = pl.pallas_call(
        functools.partial(kernel, outer_size, inner_size, shares),
        out_shape=outs,
        in_specs=[hbm] * 5,
        out_specs=[vmem] * 4,
        scratch_shapes=[
            row_block, row_block, row_block, pltpu.VMEM((heads, tokens), F32), row_block,
            pltpu.VMEM((heads, tokens), F32),
            pltpu.VMEM((heads, tokens, size), F32),
            pltpu.VMEM((heads, tokens, size), F32),
            row_block,
            pltpu.VMEM((1, size), F32),
            pltpu.VMEM((count, 1, size), F32),
            pltpu.VMEM((units, count, size), F32),
            pltpu.VMEM((2, extra, size), F32),
            pltpu.VMEM((units, 2, extra, size), F32),
            pltpu.VMEM((heads, tokens, tokens), F32),
            pltpu.VMEM((heads, tokens, tokens), BF16),
            row_block,
            pltpu.VMEM((tokens, wide), F32),
            row_block,
            pieces, pieces, pieces, pieces, sums, pieces, pieces, pieces, pieces, sums,
            pltpu.VMEM((heads, size, size), BF16),
            pltpu.VMEM((tokens, wide), F32),
            pltpu.VMEM((tokens, wide), F32),
            pltpu.SemaphoreType.DMA((5, units)),
            pltpu.SemaphoreType.DMA((4,)),
            pltpu.SemaphoreType.DMA((6, units)),
            pltpu.SemaphoreType.DMA((6, units)),
        ],
        compiler_params=pltpu.CompilerParams(
            collective_id=0, has_side_effects=True, vmem_limit_bytes=40 * 1024 * 1024),
    )(*[pltpu.with_memory_space_constraint(x, pltpu.HBM) for x in (query_rows, key_rows, value_rows, log_decay, grad_out)])
    return pl.pallas_call(
        store,
        out_shape=outs,
        in_specs=[vmem] * 4,
        out_specs=[hbm] * 4,
        scratch_shapes=[pltpu.SemaphoreType.DMA((4, 1))],
        compiler_params=pltpu.CompilerParams(vmem_limit_bytes=8 * 1024 * 1024),
    )(*results)


def solution(mesh):
    both = ("outer", "inner")
    row_spec = P(both, None)
    return jax.shard_map(
        functools.partial(body, mesh.shape["outer"], mesh.shape["inner"]),
        mesh=mesh,
        in_specs=(row_spec, row_spec, row_spec, P(None, both), row_spec),
        out_specs=(row_spec,) * 4,
        check_vma=False,
    )
```

```python
import functools
import math

import jax
import jax.numpy as jnp
from jax import lax
from jax.experimental import pallas as pl
from jax.experimental.pallas import tpu as pltpu
from jax.sharding import PartitionSpec as P

EPSILON = 1e-06
F32 = jnp.float32
BF16 = jnp.bfloat16
MESH = pl.DeviceIdType.MESH
SHARES = (2, 2, 2, 2)
UNROLL = 16
ORDER = lambda m: (-(m[1] % 2), -(m[1] // 2), -(m[0] % 2), -(m[0] // 2))


def plan(units):
    every = range(units)
    steps = [("A", 0), ("b", 0), ("f", 0), ("X", 0)]
    for u in range(1, units):
        steps += [("A", u), ("X", u)]
    steps += [("L", u) for u in every] + [("r", 0)]
    steps += [("S", u) for u in every] + [("t", 0)] + [("C", u) for u in every]
    for u in every:
        steps += [("M", u), ("Y", u), ("G", u)]
    steps += [(act, u) for act in "VWeZ" for u in every]
    return steps


def dot(a, b, da, db):
    return lax.dot_general(a, b, (((da,), (db,)), ((), ())), preferred_element_type=F32)


def kernel(outer_size, inner_size, shares, q_hbm, k_hbm, v_hbm, decay_hbm, g_hbm,
           att_ref, gq_ref, gk_ref, gv_ref,
           q_ref, k_ref, v_ref, decay_ref, g_ref,
           run_ref, col_ref, shrink_ref, qd_ref, fac_ref, facs_ref, spread_ref, prod_ref, whole_ref, dec_ref, w_ref, kd_ref, mix_ref, gm_ref,
           send1, recv1, out1, ret1, agg1, send2, recv2, out2, ret2, agg2, ent_ref, gkl_ref, gvl_ref,
           load_sems, fac_sems, send_sems, recv_sems):
    n = outer_size * inner_size
    half_inner = inner_size // 2
    count = n // 2
    heads, tokens = decay_ref.shape
    size = q_ref.shape[1] // heads
    scaling = 1.0 / math.sqrt(size)
    units = len(shares)
    first = [sum(shares[:u]) for u in range(units)]
    rows = [share * size // count for share in shares]
    lanes = size // heads
    place_o, place_i = lax.axis_index("outer"), lax.axis_index("inner")
    half = lax.div(place_i, half_inner)
    near = lax.rem(place_i, half_inner)
    seat = place_o * half_inner + near
    partner = (place_o, lax.rem(place_i + half_inner, inner_size))

    def unit_heads(u):
        return range(first[u], first[u] + shares[u])

    def unit_span(u):
        return pl.ds(first[u] * size, shares[u] * size)

    def span(h):
        return pl.ds(h * size, size)

    decay_load = pltpu.make_async_copy(decay_hbm, decay_ref, load_sems.at[0, 0])
    decay_load.start()
    loads = {}
    for at, (name, source, target) in enumerate(
            (("k", k_hbm, k_ref), ("v", v_hbm, v_ref), ("q", q_hbm, q_ref), ("g", g_hbm, g_ref))):
        for u in range(units):
            loads[name, u] = pltpu.make_async_copy(
                source.at[:, unit_span(u)], target.at[:, unit_span(u)], load_sems.at[at + 1, u])
    for u in range(units):
        loads["k", u].start()
        loads["v", u].start()

    def flipped(place, mask):
        bit = 1
        while bit <= mask:
            if mask & bit:
                place = place + bit * (1 - 2 * lax.rem(lax.div(place, bit), 2))
            bit *= 2
        return place

    binary = outer_size & (outer_size - 1) == 0 and half_inner & (half_inner - 1) == 0
    masks = [(mo, mi) for mo in range(outer_size) for mi in range(half_inner) if mo or mi]
    masks.sort(key=ORDER)

    def peers(act):
        def one(o, i):
            act(o, half * half_inner + i, o * half_inner + i)

        if binary and count <= UNROLL:
            for mo, mi in masks:
                one(flipped(place_o, mo), flipped(near, mi))
        else:
            def turn(step, carry):
                one(lax.rem(place_o + lax.rem(step + 1, outer_size), outer_size),
                    lax.rem(near + lax.div(step + 1, outer_size), half_inner))
                return carry
            lax.fori_loop(0, count - 1, turn, 0)

    barrier = pltpu.get_barrier_semaphore()
    peers(lambda o, i, s: pl.semaphore_signal(barrier, inc=1, device_id=(o, i), device_id_type=MESH))
    pl.semaphore_signal(barrier, inc=1, device_id=partner, device_id_type=MESH)

    for name in ("q", "g"):
        for u in range(units):
            loads[name, u].start()

    def seat_rows(u, s):
        return pl.ds(pl.multiple_of(first[u] * size + s * rows[u], 8), rows[u])

    def others(buffer, u):
        return buffer.at[pl.ds(first[u] * size, (count - 1) * rows[u])]

    def exchange(source, target, phase, u):
        peers(lambda o, i, s: pltpu.make_async_remote_copy(
            src_ref=source.at[seat_rows(u, s)], dst_ref=target.at[seat_rows(u, seat)],
            send_sem=send_sems.at[phase, u], recv_sem=recv_sems.at[phase, u],
            device_id=(o, i), device_id_type=MESH).start())
        target[seat_rows(u, seat)] = source[seat_rows(u, seat)]

    plain = [outer_size * sum(rows[:u]) for u in range(units)]

    def side_sums(sums, side, u):
        return sums.at[side, pl.ds(plain[u], outer_size * rows[u])]

    def across(sums, phase, u):
        pltpu.make_async_remote_copy(
            src_ref=side_sums(sums, half, u), dst_ref=side_sums(sums, half, u),
            send_sem=send_sems.at[phase, u], recv_sem=recv_sems.at[phase, u],
            device_id=partner, device_id_type=MESH).start()

    def drain(piece, sem):
        pltpu.make_async_copy(piece, piece, sem).wait()

    decay_load.wait()
    running = decay_ref[...]
    lane = lax.broadcasted_iota(jnp.int32, (heads, tokens), 1)
    shift = 1
    while shift < tokens:
        running = running + jnp.where(lane >= shift, pltpu.roll(running, shift, 1), 0.0)
        shift *= 2
    run_ref[...] = running
    totals = jnp.broadcast_to(running[:, tokens - 1:], (heads, size))
    own = lax.broadcasted_iota(jnp.int32, (heads, size), 1) // lanes == lax.broadcasted_iota(jnp.int32, (heads, size), 0)
    fac_ref[...] = jnp.exp(jnp.sum(jnp.where(own, totals, 0.0), axis=0, keepdims=True))
    facs_ref[seat] = fac_ref[...]

    def state_of(u):
        loads["k", u].wait()
        loads["v", u].wait()
        for h in unit_heads(u):
            row = running[h:h + 1]
            column = jnp.broadcast_to(row, (size, tokens)).T
            col_ref[h] = column
            total = jnp.broadcast_to(row[:, tokens - 1:], (1, size))
            cols = span(h)
            shrink = jnp.exp(total - column)
            shrink_ref[h] = shrink
            key_dec = (k_ref[:, cols].astype(F32) * shrink).astype(BF16)
            kd_ref[:, cols] = key_dec
            send1[pl.ds(h * size, size)] = dot(key_dec, v_ref[:, cols], 0, 0)

    t_index = lax.broadcasted_iota(jnp.int32, (tokens, tokens), 0)
    s_index = lax.broadcasted_iota(jnp.int32, (tokens, tokens), 1)
    causal = s_index <= t_index

    def local_mix(u):
        loads["q", u].wait()
        for h in unit_heads(u):
            cols = span(h)
            column = jnp.concatenate([col_ref[h]] * (tokens // size), axis=1)
            gaps = column - run_ref[pl.ds(h, 1)]
            decay = jnp.where(causal, jnp.exp(jnp.where(causal, gaps, 0.0)), 0.0) * scaling
            dec_ref[h] = decay
            weights = (dot(q_ref[:, cols], k_ref[:, cols], 1, 1) * decay).astype(BF16)
            w_ref[h] = weights
            mix_ref[:, cols] = dot(weights, v_ref[:, cols], 1, 0)
            qd_ref[:, cols] = (q_ref[:, cols].astype(F32) * jnp.exp(col_ref[h])).astype(BF16)

    lane_of = lax.broadcasted_iota(jnp.int32, (count, size), 1)

    def spread():
        block = facs_ref[...].reshape(count, size)
        for u in range(units):
            one = jnp.sum(jnp.where(lane_of == (first[u] + lax.div(seat * rows[u], size)) * lanes, block, 0.0), axis=1, keepdims=True)
            spread_ref[u] = jnp.broadcast_to(one, (count, size))

    def spread_products(side):
        block = prod_ref[side]
        lane_at = lax.broadcasted_iota(jnp.int32, block.shape, 1)
        for u in range(units):
            head = first[u] + lax.div(seat * rows[u], size)
            one = jnp.sum(jnp.where(lane_at == head * lanes, block, 0.0), axis=1, keepdims=True)
            whole_ref[u, side] = jnp.broadcast_to(one, block.shape)

    def factor_of(u, s):
        return spread_ref[u, pl.ds(s, 1)]

    def group_rows(sums, u, o):
        return pl.ds(plain[u] + o * rows[u], rows[u])

    def fold(source, sums, u, phase, backward):
        drain(others(source, u), recv_sems.at[phase, u])
        for o in range(outer_size):
            state = None
            for step in range(half_inner):
                s = o * half_inner + (half_inner - 1 - step if backward else step)
                term = source[seat_rows(u, s)]
                state = term if state is None else factor_of(u, s) * state + term
            sums[half, group_rows(sums, u, o)] = state
        across(sums, phase + 1, u)

    def scan(source, sums, target, result, u, phase, backward):
        drain(side_sums(sums, 1 - half, u), recv_sems.at[phase + 1, u])
        order = (1, 0) if backward else (0, 1)
        carry = jnp.zeros((rows[u], size), F32)
        for turn in range(outer_size):
            o = outer_size - 1 - turn if backward else turn
            entry = []
            for side in order:
                entry.append(carry)
                carry = whole_ref[u, side, pl.ds(o, 1)] * carry + sums[side, group_rows(sums, u, o)]
            state = jnp.where(half == order[0], entry[0], entry[1])
            for step in range(half_inner):
                s = o * half_inner + (half_inner - 1 - step if backward else step)
                target[seat_rows(u, s)] = state
                if step < half_inner - 1:
                    state = factor_of(u, s) * state + source[seat_rows(u, s)]
        exchange(target, result, phase + 2, u)

    def mix(u):
        drain(others(ret1, u), recv_sems.at[2, u])
        loads["g", u].wait()
        for h in unit_heads(u):
            cols = span(h)
            part = pl.ds(h * size, size)
            entering = ret1[part].astype(BF16)
            ent_ref[h] = entering
            query_dec = qd_ref[:, cols]
            mixed = mix_ref[:, cols] + scaling * dot(query_dec, entering, 1, 0)
            inverse = lax.rsqrt(jnp.mean(mixed * mixed, axis=1, keepdims=True) + EPSILON)
            normed = mixed * inverse
            att_ref[:, cols] = normed.astype(BF16)
            g = g_ref[:, cols].astype(F32)
            grad_mixed = (inverse * (g - normed * jnp.mean(g * normed, axis=1, keepdims=True))).astype(BF16)
            gm_ref[:, cols] = grad_mixed
            send2[part] = scaling * dot(query_dec, grad_mixed, 0, 0)

    def local_grads(u):
        for h in unit_heads(u):
            cols = span(h)
            grad_mixed = gm_ref[:, cols]
            grad_score = (dot(grad_mixed, v_ref[:, cols], 1, 1) * dec_ref[h]).astype(BF16)
            away = (scaling * jnp.exp(col_ref[h])) * dot(grad_mixed, ent_ref[h], 1, 1)
            gq_ref[:, cols] = (dot(grad_score, k_ref[:, cols], 1, 0) + away).astype(BF16)
            gkl_ref[:, cols] = dot(grad_score, q_ref[:, cols], 0, 0)
            gvl_ref[:, cols] = dot(w_ref[h], grad_mixed, 0, 0)

    def far_grads(u):
        drain(others(ret2, u), recv_sems.at[5, u])
        for h in unit_heads(u):
            cols = span(h)
            leaving = ret2[pl.ds(h * size, size)].astype(BF16)
            gk_ref[:, cols] = (gkl_ref[:, cols] + shrink_ref[h] * dot(v_ref[:, cols], leaving, 1, 1)).astype(BF16)
            gv_ref[:, cols] = (gvl_ref[:, cols] + dot(kd_ref[:, cols], leaving, 1, 0)).astype(BF16)

    def send_factors():
        peers(lambda o, i, s: pltpu.make_async_remote_copy(
            src_ref=fac_ref, dst_ref=facs_ref.at[seat],
            send_sem=fac_sems.at[0], recv_sem=fac_sems.at[1],
            device_id=(o, i), device_id_type=MESH).start())

    def take_factors():
        drain(facs_ref.at[pl.ds(0, count - 1)], fac_sems.at[1])
        prod_ref[half] = jnp.zeros(prod_ref.shape[1:], F32)
        for o in range(outer_size):
            product = facs_ref[o * half_inner]
            for step in range(1, half_inner):
                product = product * facs_ref[o * half_inner + step]
            prod_ref[half, pl.ds(o, 1)] = product
        pltpu.make_async_remote_copy(
            src_ref=prod_ref.at[half], dst_ref=prod_ref.at[half],
            send_sem=fac_sems.at[2], recv_sem=fac_sems.at[3],
            device_id=partner, device_id_type=MESH).start()
        spread()
        spread_products(half)

    def take_products():
        drain(prod_ref.at[1 - half], fac_sems.at[3])
        spread_products(1 - half)

    acts = {
        "b": lambda u: pl.semaphore_wait(barrier, count),
        "f": lambda u: send_factors(),
        "r": lambda u: take_factors(),
        "t": lambda u: take_products(),
        "A": state_of,
        "X": lambda u: exchange(send1, recv1, 0, u),
        "L": local_mix,
        "S": lambda u: fold(recv1, agg1, u, 0, False),
        "C": lambda u: scan(recv1, agg1, out1, ret1, u, 0, False),
        "M": mix,
        "Y": lambda u: exchange(send2, recv2, 3, u),
        "G": local_grads,
        "V": lambda u: fold(recv2, agg2, u, 3, True),
        "W": lambda u: scan(recv2, agg2, out2, ret2, u, 3, True),
        "Z": far_grads,
    }
    def finish_most(u):
        for phase, buffer in ((0, send1), (2, out1), (3, send2)):
            drain(others(buffer, u), send_sems.at[phase, u])
        drain(side_sums(agg1, half, u), send_sems.at[1, u])
        drain(side_sums(agg2, half, u), send_sems.at[4, u])

    acts["e"] = finish_most
    drain_factors = ((facs_ref.at[pl.ds(0, count - 1)], fac_sems.at[0]), (prod_ref.at[half], fac_sems.at[2]))
    for act, u in plan(units):
        if (act, u) == ("e", 0):
            for piece, sem in drain_factors:
                drain(piece, sem)
        acts[act](u)
    for u in range(units):
        drain(others(out2, u), send_sems.at[5, u])


def store(*refs):
    sources, targets, sems = refs[:4], refs[4:8], refs[8]
    copies = [pltpu.make_async_copy(s, t, sems.at[at]) for at, (s, t) in enumerate(zip(sources, targets))]
    for copy in copies:
        copy.start()
    for copy in copies:
        copy.wait()


def body(outer_size, inner_size, query_rows, key_rows, value_rows, log_decay, grad_out):
    n = outer_size * inner_size
    heads, tokens = log_decay.shape
    wide = query_rows.shape[1]
    size = wide // heads
    count = n // 2
    shares = SHARES
    if sum(shares) != heads or any(share * size % (8 * count) for share in shares):
        shares = (heads,)
    units = len(shares)
    extra = (outer_size + 7) // 8 * 8
    pieces = pltpu.VMEM((heads * size, size), F32)
    sums = pltpu.VMEM((2, outer_size * heads * size // count, size), F32)
    vmem = pl.BlockSpec(memory_space=pltpu.VMEM)
    hbm = pl.BlockSpec(memory_space=pltpu.HBM)
    row_block = pltpu.VMEM((tokens, wide), BF16)
    outs = [jax.ShapeDtypeStruct((tokens, wide), BF16)] * 4
    results = pl.pallas_call(
        functools.partial(kernel, outer_size, inner_size, shares),
        out_shape=outs,
        in_specs=[hbm] * 5,
        out_specs=[vmem] * 4,
        scratch_shapes=[
            row_block, row_block, row_block, pltpu.VMEM((heads, tokens), F32), row_block,
            pltpu.VMEM((heads, tokens), F32),
            pltpu.VMEM((heads, tokens, size), F32),
            pltpu.VMEM((heads, tokens, size), F32),
            row_block,
            pltpu.VMEM((1, size), F32),
            pltpu.VMEM((count, 1, size), F32),
            pltpu.VMEM((units, count, size), F32),
            pltpu.VMEM((2, extra, size), F32),
            pltpu.VMEM((units, 2, extra, size), F32),
            pltpu.VMEM((heads, tokens, tokens), F32),
            pltpu.VMEM((heads, tokens, tokens), BF16),
            row_block,
            pltpu.VMEM((tokens, wide), F32),
            row_block,
            pieces, pieces, pieces, pieces, sums, pieces, pieces, pieces, pieces, sums,
            pltpu.VMEM((heads, size, size), BF16),
            pltpu.VMEM((tokens, wide), F32),
            pltpu.VMEM((tokens, wide), F32),
            pltpu.SemaphoreType.DMA((5, units)),
            pltpu.SemaphoreType.DMA((4,)),
            pltpu.SemaphoreType.DMA((6, units)),
            pltpu.SemaphoreType.DMA((6, units)),
        ],
        compiler_params=pltpu.CompilerParams(
            collective_id=0, has_side_effects=True, vmem_limit_bytes=40 * 1024 * 1024),
    )(*[pltpu.with_memory_space_constraint(x, pltpu.HBM) for x in (query_rows, key_rows, value_rows, log_decay, grad_out)])
    return pl.pallas_call(
        store,
        out_shape=outs,
        in_specs=[vmem] * 4,
        out_specs=[hbm] * 4,
        scratch_shapes=[pltpu.SemaphoreType.DMA((4,))],
        compiler_params=pltpu.CompilerParams(vmem_limit_bytes=8 * 1024 * 1024),
    )(*results)


def solution(mesh):
    both = ("outer", "inner")
    row_spec = P(both, None)
    return jax.shard_map(
        functools.partial(body, mesh.shape["outer"], mesh.shape["inner"]),
        mesh=mesh,
        in_specs=(row_spec, row_spec, row_spec, P(None, both), row_spec),
        out_specs=(row_spec,) * 4,
        check_vma=False,
    )
```

```python
import functools
import math

import jax
import jax.numpy as jnp
from jax import lax
from jax.experimental import pallas as pl
from jax.experimental.pallas import tpu as pltpu
from jax.sharding import PartitionSpec as P

EPSILON = 1e-06
F32 = jnp.float32
BF16 = jnp.bfloat16
MESH = pl.DeviceIdType.MESH
SHARES = (2, 2, 2, 2)
UNROLL = 16
ORDER = lambda m: (-(m[1] % 2), -(m[1] // 2), -(m[0] % 2), -(m[0] // 2))


def plan(units):
    every = range(units)
    steps = [("A", 0), ("b", 0), ("f", 0), ("X", 0)]
    for u in range(1, units):
        steps += [("A", u), ("X", u)]
    steps += [("L", u) for u in every[:-1]] + [("r", 0), ("S", 0), ("L", units - 1)]
    steps += [("S", u) for u in every[1:]] + [("t", 0)] + [("C", u) for u in every]
    for u in every:
        steps += [("M", u), ("Y", u), ("G", u)]
    steps += [(act, u) for act in "VWeZ" for u in every]
    return steps


def dot(a, b, da, db):
    return lax.dot_general(a, b, (((da,), (db,)), ((), ())), preferred_element_type=F32)


def kernel(outer_size, inner_size, shares, q_hbm, k_hbm, v_hbm, decay_hbm, g_hbm,
           att_ref, gq_ref, gk_ref, gv_ref,
           q_ref, k_ref, v_ref, decay_ref, g_ref,
           run_ref, col_ref, shrink_ref, qd_ref, fac_ref, facs_ref, spread_ref, prod_ref, whole_ref, dec_ref, w_ref, kd_ref, mix_ref, gm_ref,
           send1, recv1, out1, ret1, agg1, send2, recv2, out2, ret2, agg2, ent_ref, gkl_ref, gvl_ref,
           load_sems, fac_sems, send_sems, recv_sems):
    n = outer_size * inner_size
    half_inner = inner_size // 2
    count = n // 2
    heads, tokens = decay_ref.shape
    size = q_ref.shape[1] // heads
    scaling = 1.0 / math.sqrt(size)
    units = len(shares)
    first = [sum(shares[:u]) for u in range(units)]
    rows = [share * size // count for share in shares]
    lanes = size // heads
    place_o, place_i = lax.axis_index("outer"), lax.axis_index("inner")
    half = lax.div(place_i, half_inner)
    near = lax.rem(place_i, half_inner)
    seat = place_o * half_inner + near
    partner = (place_o, lax.rem(place_i + half_inner, inner_size))

    def unit_heads(u):
        return range(first[u], first[u] + shares[u])

    def unit_span(u):
        return pl.ds(first[u] * size, shares[u] * size)

    def span(h):
        return pl.ds(h * size, size)

    decay_load = pltpu.make_async_copy(decay_hbm, decay_ref, load_sems.at[0, 0])
    decay_load.start()
    loads = {}
    for at, (name, source, target) in enumerate(
            (("k", k_hbm, k_ref), ("v", v_hbm, v_ref), ("q", q_hbm, q_ref), ("g", g_hbm, g_ref))):
        for u in range(units):
            loads[name, u] = pltpu.make_async_copy(
                source.at[:, unit_span(u)], target.at[:, unit_span(u)], load_sems.at[at + 1, u])
    for u in range(units):
        loads["k", u].start()
        loads["v", u].start()

    def flipped(place, mask):
        bit = 1
        while bit <= mask:
            if mask & bit:
                place = place + bit * (1 - 2 * lax.rem(lax.div(place, bit), 2))
            bit *= 2
        return place

    binary = outer_size & (outer_size - 1) == 0 and half_inner & (half_inner - 1) == 0
    masks = [(mo, mi) for mo in range(outer_size) for mi in range(half_inner) if mo or mi]
    masks.sort(key=ORDER)

    def peers(act):
        def one(o, i):
            act(o, half * half_inner + i, o * half_inner + i)

        if binary and count <= UNROLL:
            for mo, mi in masks:
                one(flipped(place_o, mo), flipped(near, mi))
        else:
            def turn(step, carry):
                one(lax.rem(place_o + lax.rem(step + 1, outer_size), outer_size),
                    lax.rem(near + lax.div(step + 1, outer_size), half_inner))
                return carry
            lax.fori_loop(0, count - 1, turn, 0)

    barrier = pltpu.get_barrier_semaphore()
    peers(lambda o, i, s: pl.semaphore_signal(barrier, inc=1, device_id=(o, i), device_id_type=MESH))
    pl.semaphore_signal(barrier, inc=1, device_id=partner, device_id_type=MESH)

    for name in ("q", "g"):
        for u in range(units):
            loads[name, u].start()

    def seat_rows(u, s):
        return pl.ds(pl.multiple_of(first[u] * size + s * rows[u], 8), rows[u])

    def others(buffer, u):
        return buffer.at[pl.ds(first[u] * size, (count - 1) * rows[u])]

    def exchange(source, target, phase, u):
        peers(lambda o, i, s: pltpu.make_async_remote_copy(
            src_ref=source.at[seat_rows(u, s)], dst_ref=target.at[seat_rows(u, seat)],
            send_sem=send_sems.at[phase, u], recv_sem=recv_sems.at[phase, u],
            device_id=(o, i), device_id_type=MESH).start())
        target[seat_rows(u, seat)] = source[seat_rows(u, seat)]

    plain = [outer_size * sum(rows[:u]) for u in range(units)]

    def side_sums(sums, side, u):
        return sums.at[side, pl.ds(plain[u], outer_size * rows[u])]

    def across(sums, phase, u):
        pltpu.make_async_remote_copy(
            src_ref=side_sums(sums, half, u), dst_ref=side_sums(sums, half, u),
            send_sem=send_sems.at[phase, u], recv_sem=recv_sems.at[phase, u],
            device_id=partner, device_id_type=MESH).start()

    def drain(piece, sem):
        pltpu.make_async_copy(piece, piece, sem).wait()

    decay_load.wait()
    running = decay_ref[...]
    lane = lax.broadcasted_iota(jnp.int32, (heads, tokens), 1)
    shift = 1
    while shift < tokens:
        running = running + jnp.where(lane >= shift, pltpu.roll(running, shift, 1), 0.0)
        shift *= 2
    run_ref[...] = running
    totals = jnp.broadcast_to(running[:, tokens - 1:], (heads, size))
    own = lax.broadcasted_iota(jnp.int32, (heads, size), 1) // lanes == lax.broadcasted_iota(jnp.int32, (heads, size), 0)
    fac_ref[...] = jnp.exp(jnp.sum(jnp.where(own, totals, 0.0), axis=0, keepdims=True))
    facs_ref[seat] = fac_ref[...]

    def state_of(u):
        loads["k", u].wait()
        loads["v", u].wait()
        for h in unit_heads(u):
            row = running[h:h + 1]
            column = jnp.broadcast_to(row, (size, tokens)).T
            col_ref[h] = column
            total = jnp.broadcast_to(row[:, tokens - 1:], (1, size))
            cols = span(h)
            shrink = jnp.exp(total - column)
            shrink_ref[h] = shrink
            key_dec = (k_ref[:, cols].astype(F32) * shrink).astype(BF16)
            kd_ref[:, cols] = key_dec
            send1[pl.ds(h * size, size)] = dot(key_dec, v_ref[:, cols], 0, 0)

    t_index = lax.broadcasted_iota(jnp.int32, (tokens, tokens), 0)
    s_index = lax.broadcasted_iota(jnp.int32, (tokens, tokens), 1)
    causal = s_index <= t_index

    def local_mix(u):
        loads["q", u].wait()
        for h in unit_heads(u):
            cols = span(h)
            column = jnp.concatenate([col_ref[h]] * (tokens // size), axis=1)
            gaps = column - run_ref[pl.ds(h, 1)]
            decay = jnp.where(causal, jnp.exp(jnp.where(causal, gaps, 0.0)), 0.0) * scaling
            dec_ref[h] = decay
            weights = (dot(q_ref[:, cols], k_ref[:, cols], 1, 1) * decay).astype(BF16)
            w_ref[h] = weights
            mix_ref[:, cols] = dot(weights, v_ref[:, cols], 1, 0)
            qd_ref[:, cols] = (q_ref[:, cols].astype(F32) * jnp.exp(col_ref[h])).astype(BF16)

    lane_of = lax.broadcasted_iota(jnp.int32, (count, size), 1)

    def spread():
        block = facs_ref[...].reshape(count, size)
        for u in range(units):
            one = jnp.sum(jnp.where(lane_of == (first[u] + lax.div(seat * rows[u], size)) * lanes, block, 0.0), axis=1, keepdims=True)
            spread_ref[u] = jnp.broadcast_to(one, (count, size))

    def spread_products(side):
        block = prod_ref[side]
        lane_at = lax.broadcasted_iota(jnp.int32, block.shape, 1)
        for u in range(units):
            head = first[u] + lax.div(seat * rows[u], size)
            one = jnp.sum(jnp.where(lane_at == head * lanes, block, 0.0), axis=1, keepdims=True)
            whole_ref[u, side] = jnp.broadcast_to(one, block.shape)

    def factor_of(u, s):
        return spread_ref[u, pl.ds(s, 1)]

    def group_rows(sums, u, o):
        return pl.ds(plain[u] + o * rows[u], rows[u])

    def fold(source, sums, u, phase, backward):
        drain(others(source, u), recv_sems.at[phase, u])
        for o in range(outer_size):
            state = None
            for step in range(half_inner):
                s = o * half_inner + (half_inner - 1 - step if backward else step)
                term = source[seat_rows(u, s)]
                state = term if state is None else factor_of(u, s) * state + term
            sums[half, group_rows(sums, u, o)] = state
        across(sums, phase + 1, u)

    def scan(source, sums, target, result, u, phase, backward):
        drain(side_sums(sums, 1 - half, u), recv_sems.at[phase + 1, u])
        order = (1, 0) if backward else (0, 1)
        carry = jnp.zeros((rows[u], size), F32)
        for turn in range(outer_size):
            o = outer_size - 1 - turn if backward else turn
            entry = []
            for side in order:
                entry.append(carry)
                carry = whole_ref[u, side, pl.ds(o, 1)] * carry + sums[side, group_rows(sums, u, o)]
            state = jnp.where(half == order[0], entry[0], entry[1])
            for step in range(half_inner):
                s = o * half_inner + (half_inner - 1 - step if backward else step)
                target[seat_rows(u, s)] = state
                if step < half_inner - 1:
                    state = factor_of(u, s) * state + source[seat_rows(u, s)]
        exchange(target, result, phase + 2, u)

    def mix(u):
        drain(others(ret1, u), recv_sems.at[2, u])
        loads["g", u].wait()
        for h in unit_heads(u):
            cols = span(h)
            part = pl.ds(h * size, size)
            entering = ret1[part].astype(BF16)
            ent_ref[h] = entering
            query_dec = qd_ref[:, cols]
            mixed = mix_ref[:, cols] + scaling * dot(query_dec, entering, 1, 0)
            inverse = lax.rsqrt(jnp.mean(mixed * mixed, axis=1, keepdims=True) + EPSILON)
            normed = mixed * inverse
            att_ref[:, cols] = normed.astype(BF16)
            g = g_ref[:, cols].astype(F32)
            grad_mixed = (inverse * (g - normed * jnp.mean(g * normed, axis=1, keepdims=True))).astype(BF16)
            gm_ref[:, cols] = grad_mixed
            send2[part] = scaling * dot(query_dec, grad_mixed, 0, 0)

    def local_grads(u):
        for h in unit_heads(u):
            cols = span(h)
            grad_mixed = gm_ref[:, cols]
            grad_score = (dot(grad_mixed, v_ref[:, cols], 1, 1) * dec_ref[h]).astype(BF16)
            away = (scaling * jnp.exp(col_ref[h])) * dot(grad_mixed, ent_ref[h], 1, 1)
            gq_ref[:, cols] = (dot(grad_score, k_ref[:, cols], 1, 0) + away).astype(BF16)
            gkl_ref[:, cols] = dot(grad_score, q_ref[:, cols], 0, 0)
            gvl_ref[:, cols] = dot(w_ref[h], grad_mixed, 0, 0)

    def far_grads(u):
        drain(others(ret2, u), recv_sems.at[5, u])
        for h in unit_heads(u):
            cols = span(h)
            leaving = ret2[pl.ds(h * size, size)].astype(BF16)
            gk_ref[:, cols] = (gkl_ref[:, cols] + shrink_ref[h] * dot(v_ref[:, cols], leaving, 1, 1)).astype(BF16)
            gv_ref[:, cols] = (gvl_ref[:, cols] + dot(kd_ref[:, cols], leaving, 1, 0)).astype(BF16)

    def send_factors():
        peers(lambda o, i, s: pltpu.make_async_remote_copy(
            src_ref=fac_ref, dst_ref=facs_ref.at[seat],
            send_sem=fac_sems.at[0], recv_sem=fac_sems.at[1],
            device_id=(o, i), device_id_type=MESH).start())

    def take_factors():
        drain(facs_ref.at[pl.ds(0, count - 1)], fac_sems.at[1])
        prod_ref[half] = jnp.zeros(prod_ref.shape[1:], F32)
        for o in range(outer_size):
            product = facs_ref[o * half_inner]
            for step in range(1, half_inner):
                product = product * facs_ref[o * half_inner + step]
            prod_ref[half, pl.ds(o, 1)] = product
        pltpu.make_async_remote_copy(
            src_ref=prod_ref.at[half], dst_ref=prod_ref.at[half],
            send_sem=fac_sems.at[2], recv_sem=fac_sems.at[3],
            device_id=partner, device_id_type=MESH).start()
        spread()
        spread_products(half)

    def take_products():
        drain(prod_ref.at[1 - half], fac_sems.at[3])
        spread_products(1 - half)

    acts = {
        "b": lambda u: pl.semaphore_wait(barrier, count),
        "f": lambda u: send_factors(),
        "r": lambda u: take_factors(),
        "t": lambda u: take_products(),
        "A": state_of,
        "X": lambda u: exchange(send1, recv1, 0, u),
        "L": local_mix,
        "S": lambda u: fold(recv1, agg1, u, 0, False),
        "C": lambda u: scan(recv1, agg1, out1, ret1, u, 0, False),
        "M": mix,
        "Y": lambda u: exchange(send2, recv2, 3, u),
        "G": local_grads,
        "V": lambda u: fold(recv2, agg2, u, 3, True),
        "W": lambda u: scan(recv2, agg2, out2, ret2, u, 3, True),
        "Z": far_grads,
    }
    def finish_most(u):
        for phase, buffer in ((0, send1), (2, out1), (3, send2)):
            drain(others(buffer, u), send_sems.at[phase, u])
        drain(side_sums(agg1, half, u), send_sems.at[1, u])
        drain(side_sums(agg2, half, u), send_sems.at[4, u])

    acts["e"] = finish_most
    drain_factors = ((facs_ref.at[pl.ds(0, count - 1)], fac_sems.at[0]), (prod_ref.at[half], fac_sems.at[2]))
    for act, u in plan(units):
        if (act, u) == ("e", 0):
            for piece, sem in drain_factors:
                drain(piece, sem)
        acts[act](u)
    for u in range(units):
        drain(others(out2, u), send_sems.at[5, u])


def store(*refs):
    sources, targets, sems = refs[:4], refs[4:8], refs[8]
    copies = [pltpu.make_async_copy(s, t, sems.at[at]) for at, (s, t) in enumerate(zip(sources, targets))]
    for copy in copies:
        copy.start()
    for copy in copies:
        copy.wait()


def body(outer_size, inner_size, query_rows, key_rows, value_rows, log_decay, grad_out):
    n = outer_size * inner_size
    heads, tokens = log_decay.shape
    wide = query_rows.shape[1]
    size = wide // heads
    count = n // 2
    shares = SHARES
    if sum(shares) != heads or any(share * size % (8 * count) for share in shares):
        shares = (heads,)
    units = len(shares)
    extra = (outer_size + 7) // 8 * 8
    pieces = pltpu.VMEM((heads * size, size), F32)
    sums = pltpu.VMEM((2, outer_size * heads * size // count, size), F32)
    vmem = pl.BlockSpec(memory_space=pltpu.VMEM)
    hbm = pl.BlockSpec(memory_space=pltpu.HBM)
    row_block = pltpu.VMEM((tokens, wide), BF16)
    outs = [jax.ShapeDtypeStruct((tokens, wide), BF16)] * 4
    results = pl.pallas_call(
        functools.partial(kernel, outer_size, inner_size, shares),
        out_shape=outs,
        in_specs=[hbm] * 5,
        out_specs=[vmem] * 4,
        scratch_shapes=[
            row_block, row_block, row_block, pltpu.VMEM((heads, tokens), F32), row_block,
            pltpu.VMEM((heads, tokens), F32),
            pltpu.VMEM((heads, tokens, size), F32),
            pltpu.VMEM((heads, tokens, size), F32),
            row_block,
            pltpu.VMEM((1, size), F32),
            pltpu.VMEM((count, 1, size), F32),
            pltpu.VMEM((units, count, size), F32),
            pltpu.VMEM((2, extra, size), F32),
            pltpu.VMEM((units, 2, extra, size), F32),
            pltpu.VMEM((heads, tokens, tokens), F32),
            pltpu.VMEM((heads, tokens, tokens), BF16),
            row_block,
            pltpu.VMEM((tokens, wide), F32),
            row_block,
            pieces, pieces, pieces, pieces, sums, pieces, pieces, pieces, pieces, sums,
            pltpu.VMEM((heads, size, size), BF16),
            pltpu.VMEM((tokens, wide), F32),
            pltpu.VMEM((tokens, wide), F32),
            pltpu.SemaphoreType.DMA((5, units)),
            pltpu.SemaphoreType.DMA((4,)),
            pltpu.SemaphoreType.DMA((6, units)),
            pltpu.SemaphoreType.DMA((6, units)),
        ],
        compiler_params=pltpu.CompilerParams(
            collective_id=0, has_side_effects=True, vmem_limit_bytes=40 * 1024 * 1024),
    )(*[pltpu.with_memory_space_constraint(x, pltpu.HBM) for x in (query_rows, key_rows, value_rows, log_decay, grad_out)])
    return pl.pallas_call(
        store,
        out_shape=outs,
        in_specs=[vmem] * 4,
        out_specs=[hbm] * 4,
        scratch_shapes=[pltpu.SemaphoreType.DMA((4,))],
        compiler_params=pltpu.CompilerParams(vmem_limit_bytes=8 * 1024 * 1024),
    )(*results)


def solution(mesh):
    both = ("outer", "inner")
    row_spec = P(both, None)
    return jax.shard_map(
        functools.partial(body, mesh.shape["outer"], mesh.shape["inner"]),
        mesh=mesh,
        in_specs=(row_spec, row_spec, row_spec, P(None, both), row_spec),
        out_specs=(row_spec,) * 4,
        check_vma=False,
    )
```
